512 devices in a mesh: groups: 2 (over y), ep: 32 (over z), tp: 4 (over x), dp: 2 (over core).
Axes of the slice: x: 4, y: 2, z: 32, core: 2. Of those that a mesh axis runs over, the one named last changes fastest.
The devices are a block of a 4x8x32 slice.
Arguments:
- tokens: bfloat16 [8192, 1536], P(('groups', 'ep', 'tp', 'dp')), parts along dimension 0, may hold values from -6 to 6
- expert_ids: int32 [8192, 4], P(('groups', 'ep', 'tp', 'dp')), parts along dimension 0, may hold values from 0 to 63, all different within a row; in each aligned block of 16 rows (0 to 15, 16 to 31, ...) at most 2 rows name the same one
- gate_weights: float32 [8192, 4], P(('groups', 'ep', 'tp', 'dp')), parts along dimension 0, may hold values from 0.1 to 1
- w_gate: bfloat16 [64, 1536, 1536], P(('ep', 'dp'), None, 'tp'), may hold values from -0.15625 to 0.15625
- w_up: bfloat16 [64, 1536, 1536], P(('ep', 'dp'), None, 'tp'), may hold values from -0.15625 to 0.15625
- w_down: bfloat16 [64, 1536, 1536], P(('ep', 'dp'), None, 'tp'), may hold values from -0.15625 to 0.15625
Outputs:
- mixed: bfloat16 [8192, 1536], P(('groups', 'ep', 'tp', 'dp')), parts along dimension 0
- expert_loads: int32 [128], P('groups'), parts along dimension 0
The draws below stay inside these ranges and needn't reach their ends.
There are 2 independent parts, one for each index of `groups`. The reference program is written for one: setup_inputs(seed, part) draws one part's arguments, and reference() takes and returns one part's arrays. A program takes and returns all parts, laid end to end along the dimension named above; an argument that names none is the same for every part. Nothing has to cross between parts.
Inputs may be any that keep to these rules, and one draw needn't show every extreme that they name: `expert_ids`: each row names 4 different experts. In each aligned block of 16 rows (the rows of one device) no expert is named by more than 2 rows, and in some blocks one expert is named by exactly 2 rows.
All inputs are finite; a program needn't handle non-finite values.
Results may differ from the reference program's by a relative error of at most 0.0057.
Values may be sent and summed in bfloat16 or wider, within the bound.
No kernel may reach another device: no remote copies, remote signals or barrier semaphores. Data moves between devices by JAX's collectives and lax.ppermute only.
A program may use at most 64 MiB of HBM per device.

```python
import math
import jax
import jax.numpy as jnp
import numpy as np
from jax import lax

D = 1536
FF = 1536
TOP = 4
TOK_DEV = 16
EXPERTS = 64
CAP = 2
TOKENS = 4096


def level_of(rng, shape, shards, low, largest):
    gain = 1.0
    for position, parts in shards:
        steps = jax.random.uniform(jax.random.fold_in(jax.random.fold_in(rng, 6), position), (parts,), jnp.float32, low / len(shards), largest / len(shards))
        gain = gain * jnp.repeat(jnp.exp(steps), shape[position] // parts).reshape((-1,) + (1,) * (len(shape) - 1 - position))
    return gain


def shared_out(own_key, own, number, rows, amount, top, bound, slope):
    sequence = jax.random.permutation(own_key, amount)
    crowded, ordinary = portions_of(amount, rows * top, bound, slope, True), portions_of(amount, rows * top, bound, slope, False)
    places = jnp.arange(amount)

    def named(lengths, offset_by):
        used = int((lengths > 0).sum())
        fixed = max(1, used // 4)
        passed = fixed + (places - fixed + offset_by * (used - fixed)) % max(1, amount - fixed)
        return jnp.zeros((amount,), jnp.int32).at[sequence[jnp.where(places < fixed, places, passed)]].set(jnp.asarray(lengths, jnp.int32))

    lengths = jnp.where(number % 4 == 0, named(crowded, number // 4), named(ordinary, number - number // 4 - 1))
    mixed = jax.random.permutation(jax.random.fold_in(own, 3), amount)
    donor, receiver = mixed[0:amount // 2 * 2:2], mixed[1:amount // 2 * 2:2]
    slack = jnp.minimum(lengths[donor] - 1, bound - lengths[receiver]) // 2
    slack = jnp.where((donor == sequence[0]) | (receiver == sequence[0]) | (lengths[receiver] == 0), 0, jnp.maximum(slack, 0))
    passed = jax.random.randint(jax.random.fold_in(own, 4), (amount // 2,), 0, 1 << 20) % (slack + 1)
    lengths = lengths.at[donor].add(-passed).at[receiver].add(passed)
    labels = jnp.searchsorted(jnp.cumsum(lengths), jnp.arange(rows * top), side="right").astype(jnp.int32)
    table = labels.reshape(top, rows).T
    table = table[jax.random.permutation(jax.random.fold_in(own, 1), rows)]
    offset_by = jax.random.randint(jax.random.fold_in(own, 2), (rows, 1), 0, top)
    return jnp.take_along_axis(table, (jnp.arange(top)[None, :] + offset_by) % top, axis=1)


def portions_of(amount, total, limit, skew, full):
    portions = [(1 << 20) // math.isqrt(rank ** skew) + 1 for rank in range(1, amount + 1)]
    largest = limit if full else min(limit, max(-(-total // amount), total * portions[0] // sum(portions)))
    least = 1 if total - largest >= amount - 1 else 0
    given, surplus = [largest] + [least] * (amount - 1), total - largest - least * (amount - 1)
    while surplus > 0:
        candidates = [i for i in range(1, amount) if given[i] < largest] or [i for i in range(1, amount) if given[i] < limit]
        pool, left = sum([portions[i] for i in candidates]), surplus
        for i in candidates:
            more = min(limit - given[i], max(1, left * portions[i] // pool), surplus)
            given[i] = given[i] + more
            surplus = surplus - more
    return np.array(given)


def bell_draw(own_key, shape, spread, reach, cuts=(), held_as=jnp.bfloat16):
    values = jax.random.normal(own_key, shape, jnp.float32) * spread
    if len(cuts) > 0:
        values = level_of(own_key, shape, cuts, -0.22, 0.18) * values
    return jnp.clip(values, min=-reach, max=reach).astype(held_as)


def setup_inputs(seed: int = 0, part: int = 0) -> dict:
    key_of = jax.random.split(jax.random.key(seed), 7)
    own_keys = jax.random.split(jax.random.fold_in(key_of[6], part), 7)
    tokens = bell_draw(own_keys[0], (TOKENS, D), 1.0, 6.0, ((0, 256),))
    expert_ids_keys = jax.random.split(jax.random.fold_in(own_keys[1], 1), TOKENS // TOK_DEV)
    expert_ids_turns = jax.random.permutation(jax.random.fold_in(own_keys[1], 3), TOKENS // TOK_DEV)
    expert_ids = jax.vmap(lambda own, number: shared_out(jax.random.fold_in(own_keys[1], 2), own, number, TOK_DEV, EXPERTS, TOP, CAP, 2))(expert_ids_keys, expert_ids_turns).reshape((TOKENS, TOP))
    gate_weights = jnp.clip(0.1 + 0.9 * jax.random.uniform(own_keys[2], (TOKENS, TOP), jnp.float32) ** level_of(own_keys[2], (TOKENS, TOP), ((0, 256),), -0.2, 0.2), 0.1, 1.0)
    w_gate = bell_draw(key_of[3], (EXPERTS, D, FF), D ** -0.5, 0.15625, ((0, 64), (2, 4)))
    w_up = bell_draw(key_of[4], (EXPERTS, D, FF), D ** -0.5, 0.15625, ((0, 64), (2, 4)))
    w_down = bell_draw(key_of[5], (EXPERTS, D, FF), FF ** -0.5, 0.15625, ((0, 64), (2, 4)))
    return {"tokens": tokens, "expert_ids": expert_ids, "gate_weights": gate_weights, "w_gate": w_gate, "w_up": w_up, "w_down": w_down}


def reference(tokens, expert_ids, gate_weights, w_gate, w_up, w_down):
    pair_ids = expert_ids.reshape(-1).astype(jnp.int32)
    pair_count = pair_ids.shape[0]
    expert_range = jnp.arange(EXPERTS, dtype=jnp.int32)
    onehot = (pair_ids[:, None] == expert_range[None, :]).astype(jnp.int32)
    expert_loads = jnp.sum(onehot, axis=0).astype(jnp.int32)
    earlier = (jnp.cumsum(onehot, axis=0).astype(jnp.int32) - onehot) * onehot
    slot_ranks = jnp.sum(earlier, axis=1).astype(jnp.int32)
    holder = (TOKENS // TOK_DEV) * CAP
    token_of_pair = (jnp.arange(pair_count, dtype=jnp.int32) // TOP).astype(jnp.int32)
    table = jnp.full((EXPERTS, holder), TOKENS, jnp.int32).at[pair_ids, slot_ranks].set(token_of_pair)
    padded = jnp.concatenate([tokens, jnp.zeros((1, D), jnp.bfloat16)], axis=0)

    def one_expert(packed):
        row_index, gate_part, up_part, down_part = packed
        token_rows = padded[row_index]
        gate_value = jnp.dot(token_rows, gate_part, preferred_element_type=jnp.float32)
        up_value = jnp.dot(token_rows, up_part, preferred_element_type=jnp.float32)
        hidden = (jax.nn.silu(gate_value) * up_value).astype(jnp.bfloat16)
        result = lax.dot_general(hidden, down_part, (((1,), (1,)), ((), ())), preferred_element_type=jnp.float32)
        return result.astype(jnp.bfloat16)

    outputs = lax.map(one_expert, (table, w_gate, w_up, w_down))
    picked = outputs[pair_ids, slot_ranks].reshape(TOKENS, TOP, D)
    mixed = jnp.sum(gate_weights[:, :, None] * picked.astype(jnp.float32), axis=1)
    return mixed.astype(jnp.bfloat16), expert_loads
```

```python
import jax
import jax.numpy as jnp
from jax import lax
from jax.sharding import PartitionSpec as P

EMPTY = 8.0
DIGIT = 64


def copy_for_each(array, axis):
    copies = jnp.broadcast_to(array, (lax.axis_size(axis), *array.shape))
    return lax.all_to_all(copies, axis, split_axis=0, concat_axis=0, tiled=True)


def expert_apply(token_rows, gate_part, up_part, down_part):
    gate_value = jnp.dot(token_rows, gate_part, preferred_element_type=jnp.float32)
    up_value = jnp.dot(token_rows, up_part, preferred_element_type=jnp.float32)
    hidden = (jax.nn.silu(gate_value) * up_value).astype(jnp.bfloat16)
    return lax.dot_general(
        hidden, down_part, (((1,), (1,)), ((), ())), preferred_element_type=jnp.float32
    )


def per_device(tokens, expert_ids, gate_weights, w_gate, w_up, w_down):
    tok_rows, model_width = tokens.shape
    top_count = expert_ids.shape[1]
    experts = lax.axis_size("ep") * lax.axis_size("dp")
    capacity = max(2, 2 * tok_rows * top_count // experts)
    pair_ids = expert_ids.reshape(-1)
    expert_range = jnp.arange(experts, dtype=jnp.int32)
    onehot = (pair_ids[:, None] == expert_range[None, :]).astype(jnp.int32)
    earlier = (jnp.cumsum(onehot, axis=0) - onehot) * onehot
    slot_ranks = jnp.sum(earlier, axis=1)
    targets = pair_ids * capacity + slot_ranks
    slot_range = jnp.arange(experts * capacity, dtype=jnp.int32)
    selector = jnp.any(
        targets.reshape(tok_rows, top_count)[None, :, :] == slot_range[:, None, None], axis=2
    )
    empty = ~jnp.any(selector, axis=1)
    outgoing = jnp.dot(selector.astype(jnp.bfloat16), tokens, preferred_element_type=jnp.float32)
    first = jnp.arange(model_width, dtype=jnp.int32) == 0
    outgoing = jnp.where(empty[:, None] & first[None, :], EMPTY, outgoing)
    outgoing = outgoing.astype(jnp.bfloat16).reshape(experts, capacity, model_width)
    arrived = lax.all_to_all(outgoing, ("ep", "dp"), split_axis=0, concat_axis=0, tiled=True)
    fragment = copy_for_each(arrived, "tp")
    load = jnp.sum((fragment[..., 0] < EMPTY - 1).astype(jnp.int32))
    partial_value = expert_apply(
        fragment.reshape(-1, model_width), w_gate[0], w_up[0], w_down[0]
    ).astype(jnp.bfloat16)
    partial_terms = partial_value.reshape(fragment.shape)
    terms = lax.all_to_all(partial_terms, "tp", split_axis=0, concat_axis=0, tiled=True)
    finished = jnp.sum(terms.astype(jnp.float32), axis=0).astype(jnp.bfloat16)
    digits = jnp.where(jnp.arange(128) == 0, load // DIGIT, load % DIGIT).astype(jnp.bfloat16)
    finished = jnp.concatenate(
        [finished, jnp.broadcast_to(digits, (experts, capacity, 128))], axis=2
    )
    returned = lax.all_to_all(finished, ("ep", "dp"), split_axis=0, concat_axis=0, tiled=True)
    digits = returned[:, 0, model_width : model_width + 2].astype(jnp.int32)
    expert_loads = digits[:, 0] * DIGIT + digits[:, 1]
    returned = returned.reshape(experts * capacity, -1)
    picked = jnp.take(returned, targets, axis=0)[:, :model_width]
    picked = picked.reshape(tok_rows, top_count, model_width)
    mixed = jnp.sum(gate_weights[:, :, None] * picked.astype(jnp.float32), axis=1)
    return (mixed.astype(jnp.bfloat16), expert_loads)


def solution(mesh):
    return jax.shard_map(
        per_device,
        mesh=mesh,
        in_specs=(
            P(("groups", "ep", "tp", "dp"), None),
            P(("groups", "ep", "tp", "dp"), None),
            P(("groups", "ep", "tp", "dp"), None),
            P(("ep", "dp"), None, "tp"),
            P(("ep", "dp"), None, "tp"),
            P(("ep", "dp"), None, "tp"),
        ),
        out_specs=(P(("groups", "ep", "tp", "dp"), None), P("groups")),
        check_vma=False,
    )
```

```python
import jax
import jax.numpy as jnp
from jax import lax
from jax.sharding import PartitionSpec as P

EMPTY = 8.0
DIGIT = 64


def copy_for_each(array, axis):
    copies = jnp.broadcast_to(array, (lax.axis_size(axis), *array.shape))
    return lax.all_to_all(copies, axis, split_axis=0, concat_axis=0, tiled=True)


def expert_apply(token_rows, gate_part, up_part, down_part):
    gate_value = jnp.dot(token_rows, gate_part, preferred_element_type=jnp.float32)
    up_value = jnp.dot(token_rows, up_part, preferred_element_type=jnp.float32)
    hidden = (jax.nn.silu(gate_value) * up_value).astype(jnp.bfloat16)
    return lax.dot_general(
        hidden, down_part, (((1,), (1,)), ((), ())), preferred_element_type=jnp.float32
    )


def per_device(tokens, expert_ids, gate_weights, w_gate, w_up, w_down):
    tok_rows, model_width = tokens.shape
    top_count = expert_ids.shape[1]
    experts = lax.axis_size("ep") * lax.axis_size("dp")
    capacity = max(2, 2 * tok_rows * top_count // experts)
    pair_ids = expert_ids.reshape(-1)
    expert_range = jnp.arange(experts, dtype=jnp.int32)
    onehot = (pair_ids[:, None] == expert_range[None, :]).astype(jnp.int32)
    earlier = (jnp.cumsum(onehot, axis=0) - onehot) * onehot
    slot_ranks = jnp.sum(earlier, axis=1)
    targets = pair_ids * capacity + slot_ranks
    slot_range = jnp.arange(experts * capacity, dtype=jnp.int32)
    selector = jnp.any(
        targets.reshape(tok_rows, top_count)[None, :, :] == slot_range[:, None, None], axis=2
    )
    empty = ~jnp.any(selector, axis=1)
    outgoing = jnp.dot(selector.astype(jnp.bfloat16), tokens, preferred_element_type=jnp.float32)
    first = jnp.arange(model_width, dtype=jnp.int32) == 0
    outgoing = jnp.where(empty[:, None] & first[None, :], EMPTY, outgoing)
    outgoing = outgoing.astype(jnp.bfloat16).reshape(experts, capacity, model_width)
    arrived = lax.all_to_all(outgoing, ("ep", "dp"), split_axis=0, concat_axis=0, tiled=True)
    fragment = copy_for_each(arrived.reshape(-1, model_width), "tp")
    load = jnp.sum((fragment[..., 0] < EMPTY - 1).astype(jnp.int32))
    partial_value = expert_apply(
        fragment.reshape(-1, model_width), w_gate[0], w_up[0], w_down[0]
    ).astype(jnp.bfloat16)
    partial_terms = partial_value.reshape(fragment.shape)
    terms = lax.all_to_all(partial_terms, "tp", split_axis=0, concat_axis=0, tiled=True)
    finished = jnp.sum(terms.astype(jnp.float32), axis=0).astype(jnp.bfloat16)
    digits = jnp.where(jnp.arange(128) == 0, load // DIGIT, load % DIGIT).astype(jnp.bfloat16)
    digits = jnp.broadcast_to(digits, (finished.shape[0], 128))
    finished = jnp.concatenate([finished, digits], axis=1)
    finished = finished.reshape(experts, capacity, -1)
    returned = lax.all_to_all(finished, ("ep", "dp"), split_axis=0, concat_axis=0, tiled=True)
    digits = returned[:, 0, model_width : model_width + 2].astype(jnp.int32)
    expert_loads = digits[:, 0] * DIGIT + digits[:, 1]
    returned = returned.reshape(experts * capacity, -1)
    picked = jnp.take(returned, targets, axis=0)[:, :model_width]
    picked = picked.reshape(tok_rows, top_count, model_width)
    mixed = jnp.sum(gate_weights[:, :, None] * picked.astype(jnp.float32), axis=1)
    return (mixed.astype(jnp.bfloat16), expert_loads)


def solution(mesh):
    return jax.shard_map(
        per_device,
        mesh=mesh,
        in_specs=(
            P(("groups", "ep", "tp", "dp"), None),
            P(("groups", "ep", "tp", "dp"), None),
            P(("groups", "ep", "tp", "dp"), None),
            P(("ep", "dp"), None, "tp"),
            P(("ep", "dp"), None, "tp"),
            P(("ep", "dp"), None, "tp"),
        ),
        out_specs=(P(("groups", "ep", "tp", "dp"), None), P("groups")),
        check_vma=False,
    )
```

```python
import jax
import jax.numpy as jnp
from jax import lax
from jax.experimental import pallas as pl
from jax.experimental.pallas import tpu as pltpu
from jax.sharding import PartitionSpec as P

EMPTY = 8.0
DIGIT = 64
SUBLANES, LANES = 8, 128


def shifted(array, axis, step):
    size = lax.axis_size(axis)
    return lax.ppermute(array, axis, [(i, (i + step) % size) for i in range(size)])


def expert_kernel(rows_ref, gate_ref, up_ref, down_ref, out_ref, held_ref):
    rows = rows_ref[...]
    gate_value = jnp.dot(rows, gate_ref[0], preferred_element_type=jnp.float32)
    up_value = jnp.dot(rows, up_ref[0], preferred_element_type=jnp.float32)
    hidden = (jax.nn.silu(gate_value) * up_value).astype(jnp.bfloat16)
    result = lax.dot_general(
        hidden, down_ref[0], (((1,), (1,)), ((), ())), preferred_element_type=jnp.float32
    )
    out_ref[...] = result.astype(out_ref.dtype)
    held = (rows[:, :LANES].astype(jnp.float32) < EMPTY - 1).astype(jnp.float32)
    held_ref[...] = jnp.broadcast_to(jnp.sum(held, axis=0, keepdims=True), held_ref.shape)


def expert_apply(rows, gate_part, up_part, down_part, dtype):
    count, width = rows.shape
    hidden = gate_part.shape[2]
    whole = pl.BlockSpec(memory_space=pltpu.VMEM)
    return pl.pallas_call(
        expert_kernel,
        out_shape=(
            jax.ShapeDtypeStruct((count, width), dtype),
            jax.ShapeDtypeStruct((SUBLANES, LANES), jnp.float32),
        ),
        in_specs=[whole] * 4,
        out_specs=(whole, whole),
        cost_estimate=pl.CostEstimate(
            flops=6 * count * width * hidden,
            bytes_accessed=6 * width * hidden + 4 * count * width,
            transcendentals=count * hidden,
        ),
        compiler_params=pltpu.CompilerParams(vmem_limit_bytes=16 * 2**20),
    )(rows, gate_part, up_part, down_part)


def finish_kernel(own_ref, *refs):
    *terms, out_ref = refs
    half = len(terms) // 2
    total = own_ref[...]
    for term_ref in terms[:half]:
        total = total + term_ref[...].astype(jnp.float32)
    width = total.shape[1]
    out_ref[:, :width] = total.astype(out_ref.dtype)
    load = terms[half][:1, :1]
    for held_ref in terms[half + 1 :]:
        load = load + held_ref[:1, :1]
    high = jnp.floor(load / DIGIT)
    lane = lax.broadcasted_iota(jnp.int32, (total.shape[0], LANES), 1)
    digits = jnp.where(lane == 0, high, load - high * DIGIT)
    out_ref[:, width:] = digits.astype(out_ref.dtype)


def finish(own, terms, held):
    whole = pl.BlockSpec(memory_space=pltpu.VMEM)
    return pl.pallas_call(
        finish_kernel,
        out_shape=jax.ShapeDtypeStruct((own.shape[0], own.shape[1] + LANES), jnp.bfloat16),
        in_specs=[whole] * (1 + len(terms) + len(held)),
        out_specs=whole,
        compiler_params=pltpu.CompilerParams(vmem_limit_bytes=16 * 2**20),
    )(own, *terms, *held)


def per_device(tokens, expert_ids, gate_weights, w_gate, w_up, w_down):
    tok_rows, model_width = tokens.shape
    top_count = expert_ids.shape[1]
    experts = lax.axis_size("ep") * lax.axis_size("dp")
    capacity = max(2, 2 * tok_rows * top_count // experts)
    pair_ids = expert_ids.reshape(-1)
    expert_range = jnp.arange(experts, dtype=jnp.int32)
    onehot = (pair_ids[:, None] == expert_range[None, :]).astype(jnp.int32)
    earlier = (jnp.cumsum(onehot, axis=0) - onehot) * onehot
    slot_ranks = jnp.sum(earlier, axis=1)
    targets = pair_ids * capacity + slot_ranks
    slot_range = jnp.arange(experts * capacity, dtype=jnp.int32)
    selector = jnp.any(
        targets.reshape(tok_rows, top_count)[None, :, :] == slot_range[:, None, None], axis=2
    )
    empty = ~jnp.any(selector, axis=1)
    outgoing = jnp.dot(selector.astype(jnp.bfloat16), tokens, preferred_element_type=jnp.float32)
    first = jnp.arange(model_width, dtype=jnp.int32) == 0
    outgoing = jnp.where(empty[:, None] & first[None, :], EMPTY, outgoing)
    outgoing = outgoing.astype(jnp.bfloat16).reshape(experts, capacity, model_width)
    arrived = lax.all_to_all(outgoing, ("ep", "dp"), split_axis=0, concat_axis=0, tiled=True)
    arrived = arrived.reshape(-1, model_width)
    steps = (1, lax.axis_size("tp") - 1, *range(2, lax.axis_size("tp") - 1))
    rows = [shifted(arrived, "tp", step) for step in steps]
    total, load = expert_apply(arrived, w_gate, w_up, w_down, jnp.float32)
    loads, terms = [load], []
    for step, received in zip(steps, rows, strict=True):
        partial_value, load = expert_apply(received, w_gate, w_up, w_down, jnp.bfloat16)
        loads.append(load)
        terms.append(shifted(partial_value, "tp", -step))
    finished = finish(total, terms, loads)
    finished = finished.reshape(experts, capacity, -1)
    returned = lax.all_to_all(finished, ("ep", "dp"), split_axis=0, concat_axis=0, tiled=True)
    digits = returned[:, 0, model_width : model_width + 2].astype(jnp.int32)
    expert_loads = digits[:, 0] * DIGIT + digits[:, 1]
    returned = returned.reshape(experts * capacity, -1)
    picked = jnp.take(returned, targets, axis=0)[:, :model_width]
    picked = picked.reshape(tok_rows, top_count, model_width)
    mixed = jnp.sum(gate_weights[:, :, None] * picked.astype(jnp.float32), axis=1)
    return (mixed.astype(jnp.bfloat16), expert_loads)


def solution(mesh):
    return jax.shard_map(
        per_device,
        mesh=mesh,
        in_specs=(
            P(("groups", "ep", "tp", "dp"), None),
            P(("groups", "ep", "tp", "dp"), None),
            P(("groups", "ep", "tp", "dp"), None),
            P(("ep", "dp"), None, "tp"),
            P(("ep", "dp"), None, "tp"),
            P(("ep", "dp"), None, "tp"),
        ),
        out_specs=(P(("groups", "ep", "tp", "dp"), None), P("groups")),
        check_vma=False,
    )
```

```python
import jax
import jax.numpy as jnp
from jax import lax
from jax.experimental import pallas as pl
from jax.experimental.pallas import tpu as pltpu
from jax.sharding import Mesh
from jax.sharding import PartitionSpec as P

EMPTY = 8.0
DIGIT = 64
NEAR = 2
SLOTS = 2
BLOCK = NEAR * 2
LANES = 128

f32, bf16 = jnp.float32, jnp.bfloat16
WHOLE = pl.BlockSpec(memory_space=pltpu.VMEM)
PARAMS = pltpu.CompilerParams(vmem_limit_bytes=16 * 2**20)


def iota(shape, dim):
    return lax.broadcasted_iota(jnp.int32, shape, dim)


def column(row):
    shape = (row.shape[1], row.shape[1])
    return jnp.sum(jnp.where(iota(shape, 0) == iota(shape, 1), row, 0), axis=1, keepdims=True)


def placed(ids, lanes, expert, rank, values=None):
    count = ids.shape[1]
    named = jnp.zeros((count, lanes), f32)
    value = jnp.zeros((count, lanes), f32)
    for k in range(ids.shape[0]):
        hit = column(ids[k : k + 1, :].astype(f32)).astype(jnp.int32) == expert
        named = named + jnp.where(hit, 1.0, 0.0)
        if values is not None:
            value = value + jnp.where(hit, column(values[k : k + 1, :]), 0.0)
    earlier = jnp.where(iota((count, count), 1) < iota((count, count), 0), 1.0, 0.0)
    ranks = jnp.dot(earlier.astype(bf16), named.astype(bf16), preferred_element_type=f32)
    chosen = (named > 0.5) & (ranks.astype(jnp.int32) == rank)
    return jnp.where(chosen, named if values is None else value, 0.0)


def pack_kernel(
    tokens_ref, ids_ref, weights_ref, out_ref, high_ref, low_ref, ids, weights, token_sem, ids_sem, weights_sem
):
    count, width = tokens_ref.shape
    lanes = out_ref.shape[1] - width
    token_copy = pltpu.make_async_copy(tokens_ref, out_ref.at[:, pl.ds(0, width)], token_sem)
    ids_copy = pltpu.make_async_copy(ids_ref, ids, ids_sem)
    weights_copy = pltpu.make_async_copy(weights_ref, weights, weights_sem)
    ids_copy.start()
    weights_copy.start()
    token_copy.start()
    ids_copy.wait()
    weights_copy.wait()
    lane = iota((count, lanes), 1)
    half = lanes // SLOTS
    out_ref[:, width:] = placed(ids[...], lanes, lane % half, lane // half).astype(bf16)
    slot = lane // SLOTS
    far = half // BLOCK
    mix = placed(ids[...], lanes, slot % far * BLOCK + slot // far, lane % SLOTS, weights[...])
    high = mix.astype(bf16)
    high_ref[...] = high
    low_ref[...] = (mix - high.astype(f32)).astype(bf16)
    token_copy.wait()


def select_kernel(block_ref, gathered_ref, out_ref):
    copies, count, width = out_ref.shape
    lanes = gathered_ref.shape[1] - width
    tokens = gathered_ref.shape[0]
    experts = lanes // SLOTS
    far = count // (SLOTS * BLOCK)
    row = iota((lanes, count), 1)
    lane = iota((lanes, count), 0)
    expert = block_ref[0] * BLOCK + row // (far * SLOTS)
    pick = jnp.where(lane == row % SLOTS * experts + expert, 1.0, 0.0).astype(bf16)
    chosen = jnp.dot(gathered_ref[:, width:], pick, preferred_element_type=f32)
    source = iota((tokens, count), 0) // (tokens // far)
    mine = source == iota((tokens, count), 1) // SLOTS % far
    chosen = jnp.where(mine, chosen, 0.0).astype(bf16)
    contract = (((0,), (0,)), ((), ()))
    rows = lax.dot_general(chosen, gathered_ref[:, :width], contract, preferred_element_type=f32)
    held = lax.dot_general(
        chosen, jnp.ones((tokens, LANES), bf16), contract, preferred_element_type=f32
    )
    empty = (held < 0.5) & (iota((count, LANES), 1) == 0)
    start = jnp.where(empty, EMPTY, rows[:, :LANES]).astype(bf16)
    rest = rows[:, LANES:].astype(bf16)
    for copy in range(copies):
        out_ref[copy, :, :LANES] = start
        out_ref[copy, :, LANES:] = rest


def expert_kernel(peer_ref, rows_ref, gate_ref, up_ref, down_ref, out_ref):
    count = out_ref.shape[0]
    rows = rows_ref[pl.ds(pl.multiple_of(peer_ref[0] * count, count), count), :]
    gate_value = jnp.dot(rows, gate_ref[0], preferred_element_type=f32)
    up_value = jnp.dot(rows, up_ref[0], preferred_element_type=f32)
    hidden = (jax.nn.silu(gate_value) * up_value).astype(bf16)
    result = lax.dot_general(
        hidden, down_ref[0], (((1,), (1,)), ((), ())), preferred_element_type=f32
    )
    out_ref[...] = result.astype(out_ref.dtype)


def expert_apply(peer, rows, gate_part, up_part, down_part, count, dtype):
    width, hidden = rows.shape[1], gate_part.shape[2]
    return pl.pallas_call(
        expert_kernel,
        out_shape=jax.ShapeDtypeStruct((count, width), dtype),
        in_specs=[pl.BlockSpec(memory_space=pltpu.SMEM)] + [WHOLE] * 4,
        out_specs=WHOLE,
        cost_estimate=pl.CostEstimate(
            flops=6 * count * width * hidden,
            bytes_accessed=6 * width * hidden + 4 * count * width,
            transcendentals=count * hidden,
        ),
        compiler_params=PARAMS,
    )(peer, rows, gate_part, up_part, down_part)


def finish_kernel(rows_ref, own_ref, *refs):
    *terms, out_ref = refs
    total = own_ref[...]
    for term_ref in terms:
        total = total + term_ref[...].astype(f32)
    width = total.shape[1]
    out_ref[:, :width] = total.astype(bf16)
    held = jnp.where(rows_ref[:, :LANES].astype(f32) < EMPTY - 1, 1.0, 0.0)
    load = jnp.sum(held, axis=0, keepdims=True)[:, :1]
    high = jnp.floor(load / DIGIT)
    lane = iota((total.shape[0], LANES), 1)
    out_ref[:, width:] = jnp.where(lane == 0, high, load - high * DIGIT).astype(bf16)


def mix_kernel(returned_ref, high_ref, low_ref, mixed_ref, loads_ref):
    width = mixed_ref.shape[1]
    count = returned_ref.shape[0]
    far = count // (SLOTS * BLOCK)
    rows = returned_ref[:, :width]
    mixed = jnp.dot(high_ref[...], rows, preferred_element_type=f32)
    mixed = mixed + jnp.dot(low_ref[...], rows, preferred_element_type=f32)
    mixed_ref[...] = mixed.astype(bf16)
    digits = returned_ref[:, width : width + LANES].astype(f32)
    load = digits[:, :1] * DIGIT + digits[:, 1:2]
    shape = (count, LANES)
    expert = iota(shape, 1)
    first = (expert % BLOCK * far + expert // BLOCK) * SLOTS
    load = jnp.where(iota(shape, 0) == first, load, 0.0)
    loads_ref[...] = jnp.sum(load, axis=0, keepdims=True).astype(jnp.int32)


def all_to_all(array, axis):
    return lax.all_to_all(array, axis, split_axis=0, concat_axis=0, tiled=True)


def shifted(array, axis, step):
    size = lax.axis_size(axis)
    return lax.ppermute(array, axis, [(i, (i + step) % size) for i in range(size)])


def per_device(tokens, expert_ids, gate_weights, w_gate, w_up, w_down):
    count, width = tokens.shape
    far, near = lax.axis_size("eh"), lax.axis_size("el")
    tp, dp = lax.axis_size("tp"), lax.axis_size("dp")
    experts = far * near * dp
    slots = experts * SLOTS
    steps = (*range(2, tp - 1), 1, tp - 1, 0)
    packed, high, low = pl.pallas_call(
        pack_kernel,
        out_shape=(
            jax.ShapeDtypeStruct((count, width + slots), bf16),
            jax.ShapeDtypeStruct((count, slots), bf16),
            jax.ShapeDtypeStruct((count, slots), bf16),
        ),
        in_specs=[pl.BlockSpec(memory_space=pl.ANY)] * 3,
        out_specs=(WHOLE,) * 3,
        scratch_shapes=[
            pltpu.VMEM((expert_ids.shape[1], count), jnp.int32),
            pltpu.VMEM((expert_ids.shape[1], count), f32),
            *[pltpu.SemaphoreType.DMA] * 3,
        ],
        compiler_params=PARAMS,
    )(tokens, expert_ids.T, gate_weights.T)
    me = lax.axis_index("tp").astype(jnp.int32)
    block = lax.axis_index("eh").astype(jnp.int32).reshape(1)
    peers = [((me + step) % tp).reshape(1) for step in steps]
    packed, block, *peers = lax.optimization_barrier((packed, block, *peers))
    gathered = lax.all_gather(packed, "eh", tiled=True)
    outgoing = pl.pallas_call(
        select_kernel,
        out_shape=jax.ShapeDtypeStruct((tp, slots, width), bf16),
        in_specs=[pl.BlockSpec(memory_space=pltpu.SMEM), WHOLE],
        out_specs=WHOLE,
        compiler_params=PARAMS,
    )(block, gathered)
    outgoing = outgoing.reshape(tp * near * dp, far * SLOTS, width)
    arrived = all_to_all(outgoing, ("tp", "el", "dp")).reshape(tp * slots, width)

    terms = []
    for turn, step in enumerate(steps[:-1]):
        partial_value = expert_apply(peers[turn], arrived, w_gate, w_up, w_down, slots, bf16)
        terms.append(shifted(partial_value, "tp", step))
    own = expert_apply(peers[-1], arrived, w_gate, w_up, w_down, slots, f32)
    finished = pl.pallas_call(
        finish_kernel,
        out_shape=jax.ShapeDtypeStruct((slots, width + LANES), bf16),
        in_specs=[WHOLE] * (2 + len(terms)),
        out_specs=WHOLE,
        compiler_params=PARAMS,
    )(arrived, own, *terms)
    returned = all_to_all(finished.reshape(experts, SLOTS, -1), ("el", "dp", "eh"))
    mixed, loads = pl.pallas_call(
        mix_kernel,
        out_shape=(
            jax.ShapeDtypeStruct((count, width), bf16),
            jax.ShapeDtypeStruct((1, LANES), jnp.int32),
        ),
        in_specs=[WHOLE] * 3,
        out_specs=(WHOLE, WHOLE),
        compiler_params=PARAMS,
    )(returned.reshape(slots, -1), high, low)
    return mixed, loads[0, :experts]


def solution(mesh):
    sizes = mesh.shape
    devices = mesh.devices.reshape(
        sizes["groups"], sizes["ep"] // NEAR, NEAR, sizes["tp"], sizes["dp"]
    )
    split = Mesh(devices, ("groups", "eh", "el", "tp", "dp"))
    token_spec = P(("groups", "eh", "el", "tp", "dp"), None)
    weight_spec = P(("eh", "el", "dp"), None, "tp")
    return jax.shard_map(
        per_device,
        mesh=split,
        in_specs=(token_spec,) * 3 + (weight_spec,) * 3,
        out_specs=(token_spec, P("groups")),
        check_vma=False,
    )
```

```python
import jax
import jax.numpy as jnp
from jax import lax
from jax.experimental import pallas as pl
from jax.experimental.pallas import tpu as pltpu
from jax.sharding import Mesh
from jax.sharding import PartitionSpec as P

NEAR = 2
SLOTS = 2
CORES = 2
BLOCK = NEAR * CORES
SUBLANES = 8

f32, bf16 = jnp.float32, jnp.bfloat16
WHOLE = pl.BlockSpec(memory_space=pltpu.VMEM)
PARAMS = pltpu.CompilerParams(vmem_limit_bytes=16 * 2**20)


def iota(shape, dim):
    return lax.broadcasted_iota(jnp.int32, shape, dim)


def column(row):
    shape = (row.shape[1], row.shape[1])
    return jnp.sum(jnp.where(iota(shape, 0) == iota(shape, 1), row, 0), axis=1, keepdims=True)


def placed(ids, lanes, expert, rank, values=None):
    count = ids.shape[1]
    named = jnp.zeros((count, lanes), f32)
    value = jnp.zeros((count, lanes), f32)
    for k in range(ids.shape[0]):
        hit = column(ids[k : k + 1, :].astype(f32)).astype(jnp.int32) == expert
        named = named + jnp.where(hit, 1.0, 0.0)
        if values is not None:
            value = value + jnp.where(hit, column(values[k : k + 1, :]), 0.0)
    earlier = jnp.where(iota((count, count), 1) < iota((count, count), 0), 1.0, 0.0)
    ranks = jnp.dot(earlier.astype(bf16), named.astype(bf16), preferred_element_type=f32)
    chosen = (named > 0.5) & (ranks.astype(jnp.int32) == rank)
    return jnp.where(chosen, named if values is None else value, 0.0)


def pack_kernel(
    tokens_ref, ids_ref, weights_ref, out_ref, high_ref, low_ref, ids, weights, token_sem, ids_sem, weights_sem
):
    count, width = tokens_ref.shape
    lanes = out_ref.shape[1] - width
    token_copy = pltpu.make_async_copy(tokens_ref, out_ref.at[:, pl.ds(0, width)], token_sem)
    ids_copy = pltpu.make_async_copy(ids_ref, ids, ids_sem)
    weights_copy = pltpu.make_async_copy(weights_ref, weights, weights_sem)
    ids_copy.start()
    weights_copy.start()
    token_copy.start()
    ids_copy.wait()
    weights_copy.wait()
    lane = iota((count, lanes), 1)
    half = lanes // SLOTS
    out_ref[:, width:] = placed(ids[...], lanes, lane % half, lane // half).astype(bf16)
    slot = lane // SLOTS
    chip = slot % (half // CORES)
    expert = chip // NEAR * BLOCK + chip % NEAR * CORES + slot // (half // CORES)
    mix = placed(ids[...], lanes, expert, lane % SLOTS, weights[...])
    high = mix.astype(bf16)
    high_ref[...] = high
    low_ref[...] = (mix - high.astype(f32)).astype(bf16)
    token_copy.wait()


def select_kernel(block_ref, gathered_ref, out_ref, loads_ref):
    copies, count, width = out_ref.shape
    lanes = gathered_ref.shape[1] - width
    tokens = gathered_ref.shape[0]
    experts = lanes // SLOTS
    far = count // (SLOTS * BLOCK)
    row = iota((lanes, count), 1)
    lane = iota((lanes, count), 0)
    device = row // (far * SLOTS)
    expert = block_ref[0] * BLOCK + device % NEAR * CORES + device // NEAR
    pick = jnp.where(lane == row % SLOTS * experts + expert, 1.0, 0.0).astype(bf16)
    chosen = jnp.dot(gathered_ref[:, width:], pick, preferred_element_type=f32)
    source = iota((tokens, count), 0) // (tokens // far)
    mine = source == iota((tokens, count), 1) // SLOTS % far
    chosen = jnp.where(mine, chosen, 0.0).astype(bf16)
    contract = (((0,), (0,)), ((), ()))
    rows = lax.dot_general(chosen, gathered_ref[:, :width], contract, preferred_element_type=f32)
    for copy in range(copies):
        out_ref[copy] = rows.astype(bf16)
    loads_ref[...] = jnp.dot(
        jnp.ones((loads_ref.shape[0], tokens), bf16),
        gathered_ref[:, width:],
        preferred_element_type=f32,
    )


def expert_kernel(peer_ref, rows_ref, gate_ref, up_ref, down_ref, out_ref):
    count = out_ref.shape[0]
    rows = rows_ref[pl.ds(pl.multiple_of(peer_ref[0] * count, count), count), :]
    gate_value = jnp.dot(rows, gate_ref[0], preferred_element_type=f32)
    up_value = jnp.dot(rows, up_ref[0], preferred_element_type=f32)
    hidden = (jax.nn.silu(gate_value) * up_value).astype(bf16)
    result = lax.dot_general(
        hidden, down_ref[0], (((1,), (1,)), ((), ())), preferred_element_type=f32
    )
    out_ref[...] = result.astype(out_ref.dtype)


def expert_apply(peer, rows, gate_part, up_part, down_part, count, dtype):
    width, hidden = rows.shape[1], gate_part.shape[2]
    return pl.pallas_call(
        expert_kernel,
        out_shape=jax.ShapeDtypeStruct((count, width), dtype),
        in_specs=[pl.BlockSpec(memory_space=pltpu.SMEM)] + [WHOLE] * 4,
        out_specs=WHOLE,
        cost_estimate=pl.CostEstimate(
            flops=6 * count * width * hidden,
            bytes_accessed=6 * width * hidden + 4 * count * width,
            transcendentals=count * hidden,
        ),
        compiler_params=PARAMS,
    )(peer, rows, gate_part, up_part, down_part)


def finish_kernel(own_ref, *refs):
    *terms, out_ref = refs
    total = own_ref[...]
    for term_ref in terms:
        total = total + term_ref[...].astype(f32)
    out_ref[...] = total.astype(bf16)


def mix_kernel(returned_ref, high_ref, low_ref, mixed_ref):
    rows = returned_ref[...]
    mixed = jnp.dot(high_ref[...], rows, preferred_element_type=f32)
    mixed = mixed + jnp.dot(low_ref[...], rows, preferred_element_type=f32)
    mixed_ref[...] = mixed.astype(bf16)


def all_to_all(array, axis):
    return lax.all_to_all(array, axis, split_axis=0, concat_axis=0, tiled=True)


def shifted(array, axis, step):
    size = lax.axis_size(axis)
    return lax.ppermute(array, axis, [(i, (i + step) % size) for i in range(size)])


def per_device(tokens, expert_ids, gate_weights, w_gate, w_up, w_down):
    count, width = tokens.shape
    far, near = lax.axis_size("eh"), lax.axis_size("el")
    tp, dp = lax.axis_size("tp"), lax.axis_size("dp")
    experts = far * near * dp
    slots = experts * SLOTS
    steps = (*range(2, tp - 1), 1, tp - 1, 0)
    packed, high, low = pl.pallas_call(
        pack_kernel,
        out_shape=(
            jax.ShapeDtypeStruct((count, width + slots), bf16),
            jax.ShapeDtypeStruct((count, slots), bf16),
            jax.ShapeDtypeStruct((count, slots), bf16),
        ),
        in_specs=[pl.BlockSpec(memory_space=pl.ANY)] * 3,
        out_specs=(WHOLE,) * 3,
        scratch_shapes=[
            pltpu.VMEM((expert_ids.shape[1], count), jnp.int32),
            pltpu.VMEM((expert_ids.shape[1], count), f32),
            *[pltpu.SemaphoreType.DMA] * 3,
        ],
        compiler_params=PARAMS,
    )(tokens, expert_ids.T, gate_weights.T)
    me = lax.axis_index("tp").astype(jnp.int32)
    block = lax.axis_index("eh").astype(jnp.int32).reshape(1)
    peers = [((me + step) % tp).reshape(1) for step in steps]
    packed, block, *peers = lax.optimization_barrier((packed, block, *peers))
    gathered = lax.all_gather(packed, "eh", tiled=True)
    outgoing, loads = pl.pallas_call(
        select_kernel,
        out_shape=(
            jax.ShapeDtypeStruct((tp, slots, width), bf16),
            jax.ShapeDtypeStruct((SUBLANES, slots), f32),
        ),
        in_specs=[pl.BlockSpec(memory_space=pltpu.SMEM), WHOLE],
        out_specs=(WHOLE, WHOLE),
        compiler_params=PARAMS,
    )(block, gathered)
    outgoing = outgoing.reshape(tp * dp * near, far * SLOTS, width)
    arrived = all_to_all(outgoing, ("tp", "dp", "el")).reshape(tp * slots, width)

    terms = []
    for turn, step in enumerate(steps[:-1]):
        partial_value = expert_apply(peers[turn], arrived, w_gate, w_up, w_down, slots, bf16)
        terms.append(shifted(partial_value, "tp", step))
    own = expert_apply(peers[-1], arrived, w_gate, w_up, w_down, slots, f32)
    finished = pl.pallas_call(
        finish_kernel,
        out_shape=jax.ShapeDtypeStruct((slots, width), bf16),
        in_specs=[WHOLE] * (1 + len(terms)),
        out_specs=WHOLE,
        compiler_params=PARAMS,
    )(own, *terms)
    finished = finished.reshape(dp, near, far, SLOTS, width).swapaxes(1, 2)
    returned = all_to_all(finished.reshape(experts, SLOTS, width), ("dp", "eh", "el"))

    turn = 0
    for axis in ("el", "dp", "tp"):
        step = 1
        while step < lax.axis_size(axis):
            other = shifted(loads, axis, step)
            loads = loads + other
            step, turn = 2 * step, turn + 1
    mixed = pl.pallas_call(
        mix_kernel,
        out_shape=jax.ShapeDtypeStruct((count, width), bf16),
        in_specs=[WHOLE] * 3,
        out_specs=WHOLE,
        compiler_params=PARAMS,
    )(returned.reshape(slots, width), high, low)
    loads = loads[0, :experts] + loads[0, experts:]
    return mixed, loads.astype(jnp.int32)


def solution(mesh):
    sizes = mesh.shape
    devices = mesh.devices.reshape(
        sizes["groups"], sizes["ep"] // NEAR, NEAR, sizes["tp"], sizes["dp"]
    )
    split = Mesh(devices, ("groups", "eh", "el", "tp", "dp"))
    token_spec = P(("groups", "eh", "el", "tp", "dp"), None)
    weight_spec = P(("eh", "el", "dp"), None, "tp")
    return jax.shard_map(
        per_device,
        mesh=split,
        in_specs=(token_spec,) * 3 + (weight_spec,) * 3,
        out_specs=(token_spec, P("groups")),
        check_vma=False,
    )
```

```python
import jax
import jax.numpy as jnp
from jax import lax
from jax.experimental import pallas as pl
from jax.experimental.pallas import tpu as pltpu
from jax.sharding import Mesh
from jax.sharding import PartitionSpec as P

NEAR = 2
SLOTS = 2
CORES = 2
BLOCK = NEAR * CORES
SUBLANES = 8

f32, bf16 = jnp.float32, jnp.bfloat16
WHOLE = pl.BlockSpec(memory_space=pltpu.VMEM)
PARAMS = pltpu.CompilerParams(vmem_limit_bytes=16 * 2**20)


def iota(shape, dim):
    return lax.broadcasted_iota(jnp.int32, shape, dim)


def column(row):
    shape = (row.shape[1], row.shape[1])
    return jnp.sum(jnp.where(iota(shape, 0) == iota(shape, 1), row, 0), axis=1, keepdims=True)


def placed(ids, lanes, expert, rank, values=None):
    count = ids.shape[1]
    named = jnp.zeros((count, lanes), f32)
    value = jnp.zeros((count, lanes), f32)
    for k in range(ids.shape[0]):
        hit = column(ids[k : k + 1, :].astype(f32)).astype(jnp.int32) == expert
        named = named + jnp.where(hit, 1.0, 0.0)
        if values is not None:
            value = value + jnp.where(hit, column(values[k : k + 1, :]), 0.0)
    earlier = jnp.where(iota((count, count), 1) < iota((count, count), 0), 1.0, 0.0)
    ranks = jnp.dot(earlier.astype(bf16), named.astype(bf16), preferred_element_type=f32)
    chosen = (named > 0.5) & (ranks.astype(jnp.int32) == rank)
    return jnp.where(chosen, named if values is None else value, 0.0)


def pack_kernel(tokens_ref, ids_ref, out_ref):
    width = tokens_ref.shape[1]
    lanes = out_ref.shape[1] - width
    lane = iota((tokens_ref.shape[0], lanes), 1)
    half = lanes // SLOTS
    out_ref[:, :width] = tokens_ref[...]
    out_ref[:, width:] = placed(ids_ref[...], lanes, lane % half, lane // half).astype(bf16)


def gates_kernel(ids_ref, weights_ref, high_ref, low_ref):
    lanes = high_ref.shape[1]
    lane = iota(high_ref.shape, 1)
    half = lanes // SLOTS
    slot = lane // SLOTS
    chip = slot % (half // CORES)
    expert = chip // NEAR * BLOCK + chip % NEAR * CORES + slot // (half // CORES)
    mix = placed(ids_ref[...], lanes, expert, lane % SLOTS, weights_ref[...])
    high = mix.astype(bf16)
    high_ref[...] = high
    low_ref[...] = (mix - high.astype(f32)).astype(bf16)


def select_kernel(block_ref, gathered_ref, out_ref, loads_ref):
    copies, count, width = out_ref.shape
    lanes = gathered_ref.shape[1] - width
    tokens = gathered_ref.shape[0]
    experts = lanes // SLOTS
    far = count // (SLOTS * BLOCK)
    row = iota((lanes, count), 1)
    lane = iota((lanes, count), 0)
    device = row // (far * SLOTS)
    expert = block_ref[0] * BLOCK + device % NEAR * CORES + device // NEAR
    pick = jnp.where(lane == row % SLOTS * experts + expert, 1.0, 0.0).astype(bf16)
    chosen = jnp.dot(gathered_ref[:, width:], pick, preferred_element_type=f32)
    source = iota((tokens, count), 0) // (tokens // far)
    mine = source == iota((tokens, count), 1) // SLOTS % far
    chosen = jnp.where(mine, chosen, 0.0).astype(bf16)
    contract = (((0,), (0,)), ((), ()))
    rows = lax.dot_general(chosen, gathered_ref[:, :width], contract, preferred_element_type=f32)
    for copy in range(copies):
        out_ref[copy] = rows.astype(bf16)
    loads_ref[...] = jnp.dot(
        jnp.ones((loads_ref.shape[0], tokens), bf16),
        gathered_ref[:, width:],
        preferred_element_type=f32,
    )


def expert_kernel(peer_ref, rows_ref, gate_ref, up_ref, down_ref, out_ref):
    count = out_ref.shape[0]
    rows = rows_ref[pl.ds(pl.multiple_of(peer_ref[0] * count, count), count), :]
    gate_value = jnp.dot(rows, gate_ref[0], preferred_element_type=f32)
    up_value = jnp.dot(rows, up_ref[0], preferred_element_type=f32)
    hidden = (jax.nn.silu(gate_value) * up_value).astype(bf16)
    result = lax.dot_general(
        hidden, down_ref[0], (((1,), (1,)), ((), ())), preferred_element_type=f32
    )
    out_ref[...] = result.astype(out_ref.dtype)


def expert_apply(peer, rows, gate_part, up_part, down_part, count, dtype):
    width, hidden = rows.shape[1], gate_part.shape[2]
    return pl.pallas_call(
        expert_kernel,
        out_shape=jax.ShapeDtypeStruct((count, width), dtype),
        in_specs=[pl.BlockSpec(memory_space=pltpu.SMEM)] + [WHOLE] * 4,
        out_specs=WHOLE,
        cost_estimate=pl.CostEstimate(
            flops=6 * count * width * hidden,
            bytes_accessed=6 * width * hidden + 4 * count * width,
            transcendentals=count * hidden,
        ),
        compiler_params=PARAMS,
    )(peer, rows, gate_part, up_part, down_part)


def finish_kernel(own_ref, *refs):
    *terms, out_ref = refs
    total = own_ref[...]
    for term_ref in terms:
        total = total + term_ref[...].astype(f32)
    out_ref[...] = total.astype(bf16)


def mix_kernel(returned_ref, high_ref, low_ref, mixed_ref):
    rows = returned_ref[...]
    mixed = jnp.dot(high_ref[...], rows, preferred_element_type=f32)
    mixed = mixed + jnp.dot(low_ref[...], rows, preferred_element_type=f32)
    mixed_ref[...] = mixed.astype(bf16)


def all_to_all(array, axis):
    return lax.all_to_all(array, axis, split_axis=0, concat_axis=0, tiled=True)


def shifted(array, axis, step):
    size = lax.axis_size(axis)
    return lax.ppermute(array, axis, [(i, (i + step) % size) for i in range(size)])


def per_device(tokens, expert_ids, gate_weights, w_gate, w_up, w_down):
    count, width = tokens.shape
    far, near = lax.axis_size("eh"), lax.axis_size("el")
    tp, dp = lax.axis_size("tp"), lax.axis_size("dp")
    experts = far * near * dp
    slots = experts * SLOTS
    steps = (*range(2, tp - 1), 1, tp - 1, 0)
    packed = pl.pallas_call(
        pack_kernel,
        out_shape=jax.ShapeDtypeStruct((count, width + slots), bf16),
        in_specs=[WHOLE] * 2,
        out_specs=WHOLE,
        compiler_params=PARAMS,
    )(tokens, expert_ids.T)
    me = lax.axis_index("tp").astype(jnp.int32)
    block = lax.axis_index("eh").astype(jnp.int32).reshape(1)
    peers = [((me + step) % tp).reshape(1) for step in steps]
    packed, block, *peers = lax.optimization_barrier((packed, block, *peers))
    gathered = lax.all_gather(packed, "eh", tiled=True)
    outgoing, loads = pl.pallas_call(
        select_kernel,
        out_shape=(
            jax.ShapeDtypeStruct((tp, slots, width), bf16),
            jax.ShapeDtypeStruct((SUBLANES, slots), f32),
        ),
        in_specs=[pl.BlockSpec(memory_space=pltpu.SMEM), WHOLE],
        out_specs=(WHOLE, WHOLE),
        compiler_params=PARAMS,
    )(block, gathered)
    outgoing = outgoing.reshape(tp * dp * near, far * SLOTS, width)
    arrived = all_to_all(outgoing, ("tp", "dp", "el")).reshape(tp * slots, width)

    terms = []
    for turn, step in enumerate(steps[:-1]):
        partial_value = expert_apply(peers[turn], arrived, w_gate, w_up, w_down, slots, bf16)
        terms.append(shifted(partial_value, "tp", step))
    own = expert_apply(peers[-1], arrived, w_gate, w_up, w_down, slots, f32)
    finished = pl.pallas_call(
        finish_kernel,
        out_shape=jax.ShapeDtypeStruct((slots, width), bf16),
        in_specs=[WHOLE] * (1 + len(terms)),
        out_specs=WHOLE,
        compiler_params=PARAMS,
    )(own, *terms)
    finished = finished.reshape(dp, near, far, SLOTS, width).swapaxes(1, 2)
    returned = all_to_all(finished.reshape(experts, SLOTS, width), ("dp", "eh", "el"))

    turn = 0
    for axis in ("el", "dp", "tp"):
        step = 1
        while step < lax.axis_size(axis):
            other = shifted(loads, axis, step)
            loads = loads + other
            step, turn = 2 * step, turn + 1
    high, low = pl.pallas_call(
        gates_kernel,
        out_shape=(jax.ShapeDtypeStruct((count, slots), bf16),) * 2,
        in_specs=[WHOLE] * 2,
        out_specs=(WHOLE, WHOLE),
        compiler_params=PARAMS,
    )(expert_ids.T, gate_weights.T)
    mixed = pl.pallas_call(
        mix_kernel,
        out_shape=jax.ShapeDtypeStruct((count, width), bf16),
        in_specs=[WHOLE] * 3,
        out_specs=WHOLE,
        compiler_params=PARAMS,
    )(returned.reshape(slots, width), high, low)
    loads = loads[0, :experts] + loads[0, experts:]
    return mixed, loads.astype(jnp.int32)


def solution(mesh):
    sizes = mesh.shape
    devices = mesh.devices.reshape(
        sizes["groups"], sizes["ep"] // NEAR, NEAR, sizes["tp"], sizes["dp"]
    )
    split = Mesh(devices, ("groups", "eh", "el", "tp", "dp"))
    token_spec = P(("groups", "eh", "el", "tp", "dp"), None)
    weight_spec = P(("eh", "el", "dp"), None, "tp")
    return jax.shard_map(
        per_device,
        mesh=split,
        in_specs=(token_spec,) * 3 + (weight_spec,) * 3,
        out_specs=(token_spec, P("groups")),
        check_vma=False,
    )
```

```python
import functools

import jax
import jax.numpy as jnp
from jax import lax
from jax.experimental import pallas as pl
from jax.experimental.pallas import tpu as pltpu
from jax.sharding import Mesh
from jax.sharding import PartitionSpec as P

NEAR = 2
SLOTS = 2
SUBLANES = 8

f32, bf16 = jnp.float32, jnp.bfloat16
WHOLE = pl.BlockSpec(memory_space=pltpu.VMEM)
PARAMS = pltpu.CompilerParams(vmem_limit_bytes=16 * 2**20)


def iota(shape, dim):
    return lax.broadcasted_iota(jnp.int32, shape, dim)


def column(row):
    shape = (row.shape[1], row.shape[1])
    return jnp.sum(jnp.where(iota(shape, 0) == iota(shape, 1), row, 0), axis=1, keepdims=True)


def placed(ids, lanes, expert, rank, values=None):
    count = ids.shape[1]
    named = jnp.zeros((count, lanes), f32)
    value = jnp.zeros((count, lanes), f32)
    for k in range(ids.shape[0]):
        hit = column(ids[k : k + 1, :].astype(f32)).astype(jnp.int32) == expert
        named = named + jnp.where(hit, 1.0, 0.0)
        if values is not None:
            value = value + jnp.where(hit, column(values[k : k + 1, :]), 0.0)
    earlier = jnp.where(iota((count, count), 1) < iota((count, count), 0), 1.0, 0.0)
    ranks = jnp.dot(earlier.astype(bf16), named.astype(bf16), preferred_element_type=f32)
    chosen = (named > 0.5) & (ranks.astype(jnp.int32) == rank)
    return jnp.where(chosen, named if values is None else value, 0.0)


def pack_kernel(tokens_ref, ids_ref, out_ref):
    width = tokens_ref.shape[1]
    lanes = out_ref.shape[1] - width
    lane = iota((tokens_ref.shape[0], lanes), 1)
    half = lanes // SLOTS
    out_ref[:, :width] = tokens_ref[...]
    out_ref[:, width:] = placed(ids_ref[...], lanes, lane % half, lane // half).astype(bf16)


def gates_kernel(dp, ids_ref, weights_ref, high_ref, low_ref):
    lanes = high_ref.shape[1]
    lane = iota(high_ref.shape, 1)
    half = lanes // SLOTS
    slot = lane // SLOTS
    chip = slot % (half // dp)
    expert = chip // NEAR * (NEAR * dp) + chip % NEAR * dp + slot // (half // dp)
    mix = placed(ids_ref[...], lanes, expert, lane % SLOTS, weights_ref[...])
    high = mix.astype(bf16)
    high_ref[...] = high
    low_ref[...] = (mix - high.astype(f32)).astype(bf16)


def select_kernel(dp, block_ref, gathered_ref, out_ref, loads_ref):
    copies, count, width = out_ref.shape
    lanes = gathered_ref.shape[1] - width
    tokens = gathered_ref.shape[0]
    experts = lanes // SLOTS
    far = count // (SLOTS * NEAR * dp)
    row = iota((lanes, count), 1)
    lane = iota((lanes, count), 0)
    device = row // (far * SLOTS)
    expert = block_ref[0] * (NEAR * dp) + device % NEAR * dp + device // NEAR
    pick = jnp.where(lane == row % SLOTS * experts + expert, 1.0, 0.0).astype(bf16)
    chosen = jnp.dot(gathered_ref[:, width:], pick, preferred_element_type=f32)
    source = iota((tokens, count), 0) // (tokens // far)
    mine = source == iota((tokens, count), 1) // SLOTS % far
    chosen = jnp.where(mine, chosen, 0.0).astype(bf16)
    contract = (((0,), (0,)), ((), ()))
    rows = lax.dot_general(chosen, gathered_ref[:, :width], contract, preferred_element_type=f32)
    for copy in range(copies):
        out_ref[copy] = rows.astype(bf16)
    loads_ref[...] = jnp.dot(
        jnp.ones((loads_ref.shape[0], tokens), bf16),
        gathered_ref[:, width:],
        preferred_element_type=f32,
    )


def expert_kernel(peer_ref, rows_ref, gate_ref, up_ref, down_ref, out_ref):
    count = out_ref.shape[0]
    rows = rows_ref[pl.ds(pl.multiple_of(peer_ref[0] * count, count), count), :]
    gate_value = jnp.dot(rows, gate_ref[0], preferred_element_type=f32)
    up_value = jnp.dot(rows, up_ref[0], preferred_element_type=f32)
    hidden = (jax.nn.silu(gate_value) * up_value).astype(bf16)
    result = lax.dot_general(
        hidden, down_ref[0], (((1,), (1,)), ((), ())), preferred_element_type=f32
    )
    out_ref[...] = result.astype(out_ref.dtype)


def expert_apply(peer, rows, gate_part, up_part, down_part, count, dtype):
    width, hidden = rows.shape[1], gate_part.shape[2]
    return pl.pallas_call(
        expert_kernel,
        out_shape=jax.ShapeDtypeStruct((count, width), dtype),
        in_specs=[pl.BlockSpec(memory_space=pltpu.SMEM)] + [WHOLE] * 4,
        out_specs=WHOLE,
        cost_estimate=pl.CostEstimate(
            flops=6 * count * width * hidden,
            bytes_accessed=6 * width * hidden + 4 * count * width,
            transcendentals=count * hidden,
        ),
        compiler_params=PARAMS,
    )(peer, rows, gate_part, up_part, down_part)


def finish_kernel(own_ref, *refs):
    *terms, out_ref = refs
    total = own_ref[...]
    for term_ref in terms:
        total = total + term_ref[...].astype(f32)
    out_ref[...] = total.astype(bf16)


def mix_kernel(returned_ref, high_ref, low_ref, mixed_ref):
    rows = returned_ref[...]
    mixed = jnp.dot(high_ref[...], rows, preferred_element_type=f32)
    mixed = mixed + jnp.dot(low_ref[...], rows, preferred_element_type=f32)
    mixed_ref[...] = mixed.astype(bf16)


def all_to_all(array, axis):
    return lax.all_to_all(array, axis, split_axis=0, concat_axis=0, tiled=True)


def shifted(array, axis, step):
    size = lax.axis_size(axis)
    return lax.ppermute(array, axis, [(i, (i + step) % size) for i in range(size)])


def per_device(tokens, expert_ids, gate_weights, w_gate, w_up, w_down):
    count, width = tokens.shape
    far, near = lax.axis_size("eh"), lax.axis_size("el")
    tp, dp = lax.axis_size("tp"), lax.axis_size("dp")
    experts = far * near * dp
    slots = experts * SLOTS
    steps = (*range(2, tp - 1), 1, tp - 1, 0)
    packed = pl.pallas_call(
        pack_kernel,
        out_shape=jax.ShapeDtypeStruct((count, width + slots), bf16),
        in_specs=[WHOLE] * 2,
        out_specs=WHOLE,
        compiler_params=PARAMS,
    )(tokens, expert_ids.T)
    me = lax.axis_index("tp").astype(jnp.int32)
    block = lax.axis_index("eh").astype(jnp.int32).reshape(1)
    peers = [((me + step) % tp).reshape(1) for step in steps]
    packed, block, *peers = lax.optimization_barrier((packed, block, *peers))
    gathered = lax.all_gather(packed, "eh", tiled=True)
    outgoing, loads = pl.pallas_call(
        functools.partial(select_kernel, dp),
        out_shape=(
            jax.ShapeDtypeStruct((tp, slots, width), bf16),
            jax.ShapeDtypeStruct((SUBLANES, slots), f32),
        ),
        in_specs=[pl.BlockSpec(memory_space=pltpu.SMEM), WHOLE],
        out_specs=(WHOLE, WHOLE),
        compiler_params=PARAMS,
    )(block, gathered)
    outgoing = outgoing.reshape(tp * dp * near, far * SLOTS, width)
    arrived = all_to_all(outgoing, ("tp", "dp", "el")).reshape(tp * slots, width)

    terms = []
    for turn, step in enumerate(steps[:-1]):
        partial_value = expert_apply(peers[turn], arrived, w_gate, w_up, w_down, slots, bf16)
        terms.append(shifted(partial_value, "tp", step))
    own = expert_apply(peers[-1], arrived, w_gate, w_up, w_down, slots, f32)
    finished = pl.pallas_call(
        finish_kernel,
        out_shape=jax.ShapeDtypeStruct((slots, width), bf16),
        in_specs=[WHOLE] * (1 + len(terms)),
        out_specs=WHOLE,
        compiler_params=PARAMS,
    )(own, *terms)
    finished = finished.reshape(dp, near, far, SLOTS, width).swapaxes(1, 2)
    returned = all_to_all(finished.reshape(experts, SLOTS, width), ("dp", "eh", "el"))

    turn = 0
    for axis in ("el", "dp", "tp"):
        step = 1
        while step < lax.axis_size(axis):
            other = shifted(loads, axis, step)
            loads = loads + other
            step, turn = 2 * step, turn + 1
    high, low = pl.pallas_call(
        functools.partial(gates_kernel, dp),
        out_shape=(jax.ShapeDtypeStruct((count, slots), bf16),) * 2,
        in_specs=[WHOLE] * 2,
        out_specs=(WHOLE, WHOLE),
        compiler_params=PARAMS,
    )(expert_ids.T, gate_weights.T)
    mixed = pl.pallas_call(
        mix_kernel,
        out_shape=jax.ShapeDtypeStruct((count, width), bf16),
        in_specs=[WHOLE] * 3,
        out_specs=WHOLE,
        compiler_params=PARAMS,
    )(returned.reshape(slots, width), high, low)
    loads = loads[0, :experts] + loads[0, experts:]
    return mixed, loads.astype(jnp.int32)


def solution(mesh):
    sizes = mesh.shape
    devices = mesh.devices.reshape(
        sizes["groups"], sizes["ep"] // NEAR, NEAR, sizes["tp"], sizes["dp"]
    )
    split = Mesh(devices, ("groups", "eh", "el", "tp", "dp"))
    token_spec = P(("groups", "eh", "el", "tp", "dp"), None)
    weight_spec = P(("eh", "el", "dp"), None, "tp")
    return jax.shard_map(
        per_device,
        mesh=split,
        in_specs=(token_spec,) * 3 + (weight_spec,) * 3,
        out_specs=(token_spec, P("groups")),
        check_vma=False,
    )
```
